32 devices in a mesh: node: 8 (over z, x), feat: 4 (over y, core).
Axes of the slice: x: 2, y: 2, z: 4, core: 2. Of those that a mesh axis runs over, the one named last changes fastest.
Arguments:
- features: bfloat16 [100, 8192], P('feat', 'node'), may hold values from -6 to 6
- edges_one: int32 [1024, 8192], P(None, 'node'), may hold values from 0 to 1, as said below
- w1_self: bfloat16 [100, 256], P('feat'), may hold values from -0.625 to 0.625
- w1_nbr: bfloat16 [100, 256], P('feat'), may hold values from -1.25 to 1.25
- need_blocks: int32 [8, 4], P('node'), may hold values from 0 to 7, as said below
- live_slots: int32 [8, 4], P('node'), may hold values from 0 to 1, as said below
- edges_two: int32 [4096, 8192], P(None, 'node'), may hold values from 0 to 1, as said below
- w2_self: bfloat16 [256, 47], P('feat'), may hold values from -0.375 to 0.375
- w2_nbr: bfloat16 [256, 47], P('feat'), may hold values from -0.5 to 0.5
- labels: int32 [8192], P('node'), may hold values from 0 to 46
Outputs:
- node_loss: float32 [8192], P('node')
- mean_loss: float32 [], replicated
The draws below stay inside these ranges and needn't reach their ends.
Inputs may be any that keep to these rules, and one draw needn't show every extreme that they name: `need_blocks`: row b holds 4 different blocks; its first entry is b, its second is b plus half the number of blocks, its third is b minus 1, and its entry k is b plus an offset that depends on k alone, modulo the number of blocks. `live_slots`: the first three entries of each row are 1. `edges_one`: each column has exactly 25 ones. `edges_two`: each column t has exactly 10 ones, all in rows of slots that live_slots marks as used for t's block.
All inputs are finite; a program needn't handle non-finite values.
Results may differ from the reference program's by a relative error of at most 0.00065.
Values may be sent and summed in bfloat16 or wider, within the bound.
A program may use at most 128 MiB of HBM per device.

```python
import jax
import jax.numpy as jnp
from jax import lax

F = 100
H = 256
C = 47
FAN1 = 25
FAN2 = 10
NEED = 4
BLK = 1024
NODES = 8192


def routing_tables(key):
    blocks = NODES // BLK
    offsets = jnp.arange(blocks, dtype=jnp.int32)
    scores = jax.random.randint(jax.random.fold_in(key, 12), (blocks,), 0, 2 ** 20) * blocks + offsets
    scores = jnp.where(offsets == blocks - 1, 2 ** 30 - 2, scores)
    scores = jnp.where(offsets == blocks // 2, 2 ** 30 - 1, scores)
    scores = jnp.where(offsets == 0, 2 ** 30, scores)
    chosen = lax.top_k(scores, NEED)[1].astype(jnp.int32)
    need = (jnp.arange(blocks, dtype=jnp.int32)[:, None] + chosen[None, :]) % blocks
    level = jax.random.randint(jax.random.fold_in(key, 13), (blocks, 1), 0, NEED + 1)
    coins = jax.random.randint(jax.random.fold_in(key, 14), (blocks, NEED), 0, NEED)
    slots = jnp.arange(NEED, dtype=jnp.int32)[None, :]
    live = jnp.where((slots < 3) | (coins < level), 1, 0).astype(jnp.int32)
    return (need.astype(jnp.int32), live)


def draw_need_blocks(key, part):
    return routing_tables(key)[0]


def draw_live_slots(key, part):
    return routing_tables(key)[1]


def draw_edges_two(key, part):
    need, live = routing_tables(key)
    width = NEED * BLK
    rows = jnp.arange(width, dtype=jnp.int32)[None, :]
    targets = jnp.arange(NODES, dtype=jnp.int32)
    used = live[targets // BLK][:, rows[0] // BLK]
    scores = jax.random.randint(jax.random.fold_in(key, 15), (NODES, width), 0, 2 ** 18) * width + rows
    scores = jnp.where(used == 1, scores, scores - 2 ** 30)
    chosen = lax.top_k(scores, FAN2)[1].astype(jnp.int32)
    return jnp.zeros((width, NODES), jnp.int32).at[chosen, targets[:, None]].set(1)


def draw_edges_one(key, part):
    rows = jnp.arange(BLK, dtype=jnp.int32)[None, :]
    targets = jnp.arange(NODES, dtype=jnp.int32)
    scores = jax.random.randint(jax.random.fold_in(key, 21), (NODES, BLK), 0, 2 ** 18) * BLK + rows
    chosen = lax.top_k(scores, FAN1)[1].astype(jnp.int32)
    return jnp.zeros((BLK, NODES), jnp.int32).at[chosen, targets[:, None]].set(1)


def place_ends(values, rng, least, top_value):
    spot = [jax.random.randint(jax.random.fold_in(rng, axis), (), 0, length) for axis, length in enumerate(values.shape)]
    longest = values.shape.index(max(values.shape))
    next_to = spot[:longest] + [(spot[longest] + 1) % values.shape[longest]] + spot[longest + 1:]
    return values.at[tuple(spot)].set(least).at[tuple(next_to)].set(top_value)


def levels(own_key, extent, shards, least, high):
    def one(axis_at, shards_of):
        heights = jax.random.uniform(jax.random.fold_in(jax.random.fold_in(own_key, 6), axis_at), (shards_of,), jnp.float32, least / len(shards), high / len(shards))
        return jnp.repeat(jnp.exp(heights), extent[axis_at] // shards_of).reshape((-1,) + (1,) * (len(extent) - axis_at - 1))

    level = one(*shards[0])
    for cut in shards[1:]:
        level = level * one(*cut)
    return level


def normal_values(stream_key, dims, deviation, most, split=(), kind=jnp.bfloat16):
    level = levels(stream_key, dims, split, -0.22, 0.18) if split else 1.0
    values = jax.random.normal(stream_key, dims, jnp.float32) * deviation * level
    return jnp.minimum(jnp.maximum(values, -most), most).astype(kind)


def setup_inputs(seed: int = 0) -> dict:
    keys = jax.random.split(jax.random.key(seed), 11)
    features = normal_values(keys[0], (F, NODES), 1.0, 6.0, ((0, 4), (1, 8)))
    edges_one = draw_edges_one(jax.random.fold_in(keys[10], 71), 0)
    w1_self = normal_values(keys[2], (F, H), F ** -0.5, 0.625, ((0, 4),))
    w1_nbr = normal_values(keys[3], (F, H), (F // 4) ** -0.5, 1.25, ((0, 4),))
    need_blocks = draw_need_blocks(jax.random.fold_in(keys[10], 71), 0)
    live_slots = draw_live_slots(jax.random.fold_in(keys[10], 71), 0)
    edges_two = draw_edges_two(jax.random.fold_in(keys[10], 71), 0)
    w2_self = normal_values(keys[7], (H, C), H ** -0.5, 0.375, ((0, 4),))
    w2_nbr = normal_values(keys[8], (H, C), (H // 2) ** -0.5, 0.5, ((0, 4),))
    labels = place_ends(jax.random.randint(keys[9], (NODES,), 0, C), jax.random.fold_in(keys[9], 1), 0, C - 1).astype(jnp.int32)
    return {"features": features, "edges_one": edges_one, "w1_self": w1_self, "w1_nbr": w1_nbr, "need_blocks": need_blocks, "live_slots": live_slots, "edges_two": edges_two, "w2_self": w2_self, "w2_nbr": w2_nbr, "labels": labels}


def reference(features, edges_one, w1_self, w1_nbr, need_blocks, live_slots, edges_two, w2_self, w2_nbr, labels):
    blocks = NODES // BLK
    inputs = features.reshape(F, blocks, BLK).transpose(1, 0, 2)
    firsts = edges_one.reshape(BLK, blocks, BLK).transpose(1, 0, 2)

    def first_layer(pair):
        block_x, adjacency = pair
        neighbour = (jnp.dot(block_x, adjacency.astype(jnp.bfloat16), preferred_element_type=jnp.float32) / FAN1).astype(jnp.bfloat16)
        before = jnp.dot(w1_self.T, block_x, preferred_element_type=jnp.float32)
        before = before + jnp.dot(w1_nbr.T, neighbour, preferred_element_type=jnp.float32)
        return jax.nn.relu(before).astype(jnp.bfloat16)

    hidden = lax.map(first_layer, (inputs, firsts))

    def second_layer(block):
        columns = lax.dynamic_slice_in_dim(edges_two, block * BLK, BLK, 1).reshape(NEED, BLK, BLK).astype(jnp.float32)
        weights = live_slots[block].astype(jnp.float32)
        sources = hidden[need_blocks[block]].astype(jnp.float32) * weights[:, None, None]
        gathered = jnp.einsum("khs,kst->ht", sources, columns, precision=lax.Precision.HIGHEST)
        logits = jnp.dot(w2_self.T, hidden[block], preferred_element_type=jnp.float32)
        logits = logits + jnp.dot(w2_nbr.T.astype(jnp.float32), gathered, precision=lax.Precision.HIGHEST) / FAN2
        block_labels = lax.dynamic_slice_in_dim(labels, block * BLK, BLK)
        class_ids = jnp.arange(C, dtype=jnp.int32)[:, None]
        picked = jnp.sum(jnp.where(class_ids == block_labels[None, :], logits, 0.0), 0)
        return jnp.log(jnp.sum(jnp.exp(logits), 0)) - picked

    node_loss = lax.map(second_layer, jnp.arange(blocks, dtype=jnp.int32)).reshape(NODES)
    mean_loss = jnp.sum(node_loss) / NODES
    return node_loss, mean_loss
```

```python
import functools

import jax
import jax.numpy as jnp
from jax import lax
from jax.experimental import pallas as pl
from jax.experimental.pallas import tpu as pltpu
from jax.sharding import PartitionSpec as P

FAN1 = 25
FAN2 = 10
MESH = pl.DeviceIdType.MESH


def kernel(
    nodes,
    feats,
    features,
    edges_one,
    w1_self,
    w1_nbr,
    need,
    live,
    edges_two,
    w2_self,
    w2_nbr,
    labels,
    loss_out,
    mean_out,
    feat_full,
    edge1,
    edge2,
    lab,
    w1s_all,
    w1n_all,
    w2s_all,
    w2n_all,
    feat_all,
    agg_own,
    agg_all,
    p_all,
    part,
    part_all,
    loss_all,
    load_sem,
    edge1_sem,
    edge2_sem,
    a_send,
    a_recv,
    p_send,
    p_recv,
    c_send,
    c_recv,
    d_send,
    d_recv,
):
    node = lax.axis_index("node")
    feat = lax.axis_index("feat")
    block = feat_full.shape[1]
    quarter = block // feats
    slots = edges_two.shape[0] // block
    e1_chunks = edge1.shape[0]
    e1_rows = edge1.shape[1]

    def cols(index):
        return pl.ds(pl.multiple_of(index * quarter, quarter), quarter)

    def remote(src, dst, send, recv, node_id, feat_id):
        return pltpu.make_async_remote_copy(
            src_ref=src,
            dst_ref=dst,
            send_sem=send,
            recv_sem=recv,
            device_id={"node": node_id, "feat": feat_id},
            device_id_type=MESH,
        )

    loads = [
        pltpu.make_async_copy(features, feat_full, load_sem.at[0]),
        pltpu.make_async_copy(w1_self, w1s_all.at[feat], load_sem.at[1]),
        pltpu.make_async_copy(w1_nbr, w1n_all.at[feat], load_sem.at[2]),
        pltpu.make_async_copy(w2_self, w2s_all.at[feat], load_sem.at[3]),
        pltpu.make_async_copy(w2_nbr, w2n_all.at[feat], load_sem.at[4]),
        pltpu.make_async_copy(labels, lab, load_sem.at[5]),
    ]
    for copy in loads:
        copy.start()
    e1_loads = [
        pltpu.make_async_copy(
            edges_one.at[pl.ds(c * e1_rows, e1_rows), :], edge1.at[c], edge1_sem.at[c]
        )
        for c in range(e1_chunks)
    ]
    for copy in e1_loads:
        copy.start()
    e2_loads = [
        pltpu.make_async_copy(
            edges_two.at[pl.ds(pl.multiple_of(k * block + feat * quarter, quarter), quarter), :],
            edge2.at[k],
            edge2_sem.at[k],
        )
        for k in range(slots)
    ]
    for copy in e2_loads:
        copy.start()

    barrier = pltpu.get_barrier_semaphore()
    others = [
        (dn, df) for dn in range(nodes) for df in range(feats) if dn or df
    ]
    for dn, df in others:
        pl.semaphore_signal(
            barrier,
            inc=1,
            device_id={
                "node": lax.rem(node + dn, nodes),
                "feat": lax.rem(feat + df, feats),
            },
            device_id_type=MESH,
        )

    loads[0].wait()
    total = None
    for c in range(e1_chunks):
        e1_loads[c].wait()
        term = jnp.dot(
            feat_full[:, c * e1_rows : (c + 1) * e1_rows],
            edge1[c].astype(jnp.bfloat16),
            preferred_element_type=jnp.float32,
        )
        total = term if total is None else total + term
    agg_own[...] = (total / FAN1).astype(jnp.bfloat16)
    for copy in loads[1:]:
        copy.wait()

    pl.semaphore_wait(barrier, len(others))

    sent = []
    arrivals = {}
    groups = [
        (0, lambda to: feat_full.at[:, cols(to)], lambda who: feat_all.at[who]),
        (1, lambda to: agg_own.at[:, cols(to)], lambda who: agg_all.at[who]),
        (2, lambda to: w1s_all.at[feat], lambda who: w1s_all.at[who]),
        (3, lambda to: w1n_all.at[feat], lambda who: w1n_all.at[who]),
        (4, lambda to: w2n_all.at[feat], lambda who: w2n_all.at[who]),
        (5, lambda to: w2s_all.at[feat], lambda who: w2s_all.at[who]),
    ]
    for item, source, target in groups:
        for df in range(1, feats):
            to = lax.rem(feat + df, feats)
            come = lax.rem(feat + feats - df, feats)
            copy = remote(
                source(to), target(feat), a_send.at[item, df], a_recv.at[item, df], node, to
            )
            copy.start()
            sent.append(copy)
            arrivals[item, df] = remote(
                source(to), target(come), a_send.at[item, df], a_recv.at[item, df], node, to
            )

    def contract(weight, values):
        return lax.dot_general(
            weight, values, (((0,), (0,)), ((), ())), preferred_element_type=jnp.float32
        )

    before = contract(w1s_all[feat], feat_full[:, cols(feat)])
    before = before + contract(w1n_all[feat], agg_own[:, cols(feat)])
    for df in range(1, feats):
        come = lax.rem(feat + feats - df, feats)
        arrivals[0, df].wait_recv()
        arrivals[2, df].wait_recv()
        before = before + contract(w1s_all[come], feat_all[come])
        arrivals[1, df].wait_recv()
        arrivals[3, df].wait_recv()
        before = before + contract(w1n_all[come], agg_all[come])
    hidden = jnp.maximum(before, 0.0).astype(jnp.bfloat16)

    share = hidden.shape[0] // feats
    for df in range(1, feats):
        arrivals[4, df].wait_recv()
    projected = None
    for who in range(feats):
        term = jnp.dot(
            w2n_all[who],
            hidden[who * share : (who + 1) * share],
            preferred_element_type=jnp.float32,
        )
        projected = term if projected is None else projected + term
    p_all[node] = projected.astype(p_all.dtype)

    p_arrive = {}
    for dn in range(1, nodes):
        to = lax.rem(node + dn, nodes)
        come = lax.rem(node + nodes - dn, nodes)
        copy = remote(p_all.at[node], p_all.at[node], p_send.at[dn], p_recv.at[dn], to, feat)
        copy.start()
        sent.append(copy)
        p_arrive[dn] = remote(
            p_all.at[node], p_all.at[come], p_send.at[dn], p_recv.at[dn], to, feat
        )

    for df in range(1, feats):
        arrivals[5, df].wait_recv()
    self_term = None
    for who in range(feats):
        term = jnp.dot(
            w2s_all[who],
            hidden[who * share : (who + 1) * share],
            preferred_element_type=jnp.float32,
        )
        self_term = term if self_term is None else self_term + term

    def gather(k, values):
        return jnp.dot(
            values, edge2[k].astype(jnp.bfloat16), preferred_element_type=jnp.float32
        )

    e2_loads[0].wait()
    gathered = gather(0, p_all[node])
    half = nodes // 2
    e2_loads[2].wait()
    p_arrive[1].wait_recv()
    gathered = gathered + gather(2, p_all[lax.rem(node + nodes - 1, nodes)])
    e2_loads[1].wait()
    if half != 1:
        p_arrive[half].wait_recv()
    gathered = gathered + gather(1, p_all[lax.rem(node + half, nodes)])
    for dn in range(1, nodes):
        if dn not in (1, half):
            p_arrive[dn].wait_recv()
    for k in range(3, slots):
        e2_loads[k].wait()
        values = p_all[need[0, k]]
        values = jnp.where(live[0, k] == 1, values, jnp.zeros_like(values))
        gathered = gathered + gather(k, values)
    part[...] = gathered

    c_arrive = {}
    for df in range(1, feats):
        to = lax.rem(feat + df, feats)
        come = lax.rem(feat + feats - df, feats)
        copy = remote(
            part.at[:, cols(to)], part_all.at[feat], c_send.at[df], c_recv.at[df], node, to
        )
        copy.start()
        sent.append(copy)
        c_arrive[df] = remote(
            part.at[:, cols(to)], part_all.at[come], c_send.at[df], c_recv.at[df], node, to
        )
    summed = part[:, cols(feat)]
    for df in range(1, feats):
        come = lax.rem(feat + feats - df, feats)
        c_arrive[df].wait_recv()
        summed = summed + part_all[come]
    logits = self_term + summed / FAN2
    class_ids = lax.broadcasted_iota(jnp.int32, logits.shape, 0)
    picked = jnp.sum(
        jnp.where(class_ids == lab[:, cols(feat)], logits, 0.0), axis=0, keepdims=True
    )
    loss = jnp.log(jnp.sum(jnp.exp(logits), axis=0, keepdims=True)) - picked
    mine = node * feats + feat
    loss_all[mine] = loss

    d_arrive = []
    for index, (dn, df) in enumerate(others):
        to_node = lax.rem(node + dn, nodes)
        to_feat = lax.rem(feat + df, feats)
        come = lax.rem(node + nodes - dn, nodes) * feats + lax.rem(feat + feats - df, feats)
        copy = remote(
            loss_all.at[mine], loss_all.at[mine], d_send.at[index], d_recv.at[index], to_node, to_feat
        )
        copy.start()
        sent.append(copy)
        d_arrive.append(
            remote(
                loss_all.at[mine], loss_all.at[come], d_send.at[index], d_recv.at[index], to_node, to_feat
            )
        )
    for copy in d_arrive:
        copy.wait_recv()
    for who in range(feats):
        loss_out[:, who * quarter : (who + 1) * quarter] = loss_all[node * feats + who]
    total_loss = jnp.sum(loss_all[...])
    mean_out[0, 0] = total_loss / (block * nodes)
    for copy in sent:
        copy.wait_send()


def local(nodes, feats, features, edges_one, w1_self, w1_nbr, need, live, edges_two, w2_self, w2_nbr, labels):
    rows, block = features.shape
    hidden = w1_self.shape[1]
    share, classes = w2_self.shape
    quarter = block // feats
    slots = need.shape[1]
    chunks = 4
    ndev = nodes * feats
    bf16, f32, i32 = jnp.bfloat16, jnp.float32, jnp.int32
    anywhere = pl.BlockSpec(memory_space=pl.ANY)
    scalar = pl.BlockSpec(memory_space=pltpu.SMEM)
    sems = pltpu.SemaphoreType.DMA
    loss, mean = pl.pallas_call(
        functools.partial(kernel, nodes, feats),
        out_shape=(
            jax.ShapeDtypeStruct((1, block), f32),
            jax.ShapeDtypeStruct((1, 1), f32),
        ),
        in_specs=[
            anywhere,
            anywhere,
            anywhere,
            anywhere,
            scalar,
            scalar,
            anywhere,
            anywhere,
            anywhere,
            anywhere,
        ],
        out_specs=(pl.BlockSpec(memory_space=pltpu.VMEM), scalar),
        scratch_shapes=[
            pltpu.VMEM((rows, block), bf16),
            pltpu.VMEM((chunks, block // chunks, block), i32),
            pltpu.VMEM((slots, quarter, block), i32),
            pltpu.VMEM((1, block), i32),
            pltpu.VMEM((feats, rows, hidden), bf16),
            pltpu.VMEM((feats, rows, hidden), bf16),
            pltpu.VMEM((feats, classes, share), bf16),
            pltpu.VMEM((feats, classes, share), bf16),
            pltpu.VMEM((feats, rows, quarter), bf16),
            pltpu.VMEM((rows, block), bf16),
            pltpu.VMEM((feats, rows, quarter), bf16),
            pltpu.VMEM((nodes, classes, quarter), bf16),
            pltpu.VMEM((classes, block), f32),
            pltpu.VMEM((feats, classes, quarter), f32),
            pltpu.VMEM((ndev, 1, quarter), f32),
            sems((6,)),
            sems((chunks,)),
            sems((slots,)),
            sems((6, feats)),
            sems((6, feats)),
            sems((nodes,)),
            sems((nodes,)),
            sems((feats,)),
            sems((feats,)),
            sems((ndev,)),
            sems((ndev,)),
        ],
        compiler_params=pltpu.CompilerParams(
            collective_id=0,
            has_side_effects=True,
            vmem_limit_bytes=40 * 1024 * 1024,
        ),
    )(
        features,
        edges_one,
        w1_self,
        w1_nbr,
        need,
        live,
        edges_two,
        w2_self.T,
        w2_nbr.T,
        labels.reshape(1, block),
    )
    return loss.reshape(block), mean.reshape(())


def solution(mesh):
    return jax.shard_map(
        functools.partial(local, mesh.shape["node"], mesh.shape["feat"]),
        mesh=mesh,
        in_specs=(
            P("feat", "node"),
            P(None, "node"),
            P("feat", None),
            P("feat", None),
            P("node", None),
            P("node", None),
            P(None, "node"),
            P("feat", None),
            P("feat", None),
            P("node"),
        ),
        out_specs=(P("node"), P()),
        check_vma=False,
    )
```

```python
import functools

import jax
import jax.numpy as jnp
from jax import lax
from jax.experimental import pallas as pl
from jax.experimental.pallas import tpu as pltpu
from jax.sharding import PartitionSpec as P

FAN1 = 25
FAN2 = 10
MESH = pl.DeviceIdType.MESH


def kernel(
    nodes,
    feats,
    features,
    edges_one,
    w1_self,
    w1_nbr,
    need,
    live,
    edges_two,
    w2_self,
    w2_nbr,
    labels,
    loss_out,
    mean_out,
    feat_full,
    edge1,
    edge2,
    lab,
    w1s_all,
    w1n_all,
    w2s_all,
    w2n_all,
    feat_all,
    agg_own,
    agg_all,
    p_all,
    part,
    part_all,
    loss_all,
    load_sem,
    edge1_sem,
    edge2_sem,
    a_send,
    a_recv,
    p_send,
    p_recv,
    c_send,
    c_recv,
    d_send,
    d_recv,
    ready,
):
    node = lax.axis_index("node")
    feat = lax.axis_index("feat")
    block = feat_full.shape[1]
    quarter = block // feats
    slots = edges_two.shape[0] // block
    e1_chunks = edge1.shape[0]
    e1_rows = edge1.shape[1]

    def cols(index):
        return pl.ds(pl.multiple_of(index * quarter, quarter), quarter)

    def remote(src, dst, send, recv, node_id, feat_id):
        return pltpu.make_async_remote_copy(
            src_ref=src,
            dst_ref=dst,
            send_sem=send,
            recv_sem=recv,
            device_id={"node": node_id, "feat": feat_id},
            device_id_type=MESH,
        )

    loads = [
        pltpu.make_async_copy(features, feat_full, load_sem.at[0]),
        pltpu.make_async_copy(w1_self, w1s_all.at[feat], load_sem.at[1]),
        pltpu.make_async_copy(w1_nbr, w1n_all.at[feat], load_sem.at[2]),
        pltpu.make_async_copy(w2_self, w2s_all.at[feat], load_sem.at[3]),
        pltpu.make_async_copy(w2_nbr, w2n_all.at[feat], load_sem.at[4]),
        pltpu.make_async_copy(labels, lab, load_sem.at[5]),
    ]
    for copy in loads:
        copy.start()
    e1_loads = [
        pltpu.make_async_copy(
            edges_one.at[pl.ds(c * e1_rows, e1_rows), :], edge1.at[c], edge1_sem.at[c]
        )
        for c in range(e1_chunks)
    ]
    for copy in e1_loads:
        copy.start()
    e2_loads = [
        pltpu.make_async_copy(
            edges_two.at[pl.ds(pl.multiple_of(k * block + feat * quarter, quarter), quarter), :],
            edge2.at[k],
            edge2_sem.at[k],
        )
        for k in range(slots)
    ]
    barrier = pltpu.get_barrier_semaphore()
    odd = lax.rem(feat, 2)
    partner = feat + 1 - 2 * odd

    def greet(semaphore, to_node, to_feat):
        pl.semaphore_signal(
            semaphore,
            inc=1,
            device_id={"node": to_node, "feat": to_feat},
            device_id_type=MESH,
        )

    for df in range(1, feats):
        to = lax.rem(feat + df, feats)
        pl.when(lax.rem(to, 2) == 0)(functools.partial(greet, barrier, node, to))
    for dn in range(1, nodes):
        greet(barrier, lax.rem(node + dn, nodes), feat + 1 - odd)

    def hear(count):
        pl.semaphore_wait(barrier, count)
        greet(ready, node, partner)

    for copy in loads:
        copy.wait()
    pl.when(odd == 0)(functools.partial(hear, feats - 1))
    pl.when(odd == 1)(lambda: pl.semaphore_wait(ready, 1))

    sent = []
    arrivals = {}
    groups = [
        (0, lambda to: feat_full.at[:, cols(to)], lambda who: feat_all.at[who]),
        (1, lambda to: agg_own.at[:, cols(to)], lambda who: agg_all.at[who]),
        (2, lambda to: w1s_all.at[feat], lambda who: w1s_all.at[who]),
        (3, lambda to: w1n_all.at[feat], lambda who: w1n_all.at[who]),
        (4, lambda to: w2n_all.at[feat], lambda who: w2n_all.at[who]),
        (5, lambda to: w2s_all.at[feat], lambda who: w2s_all.at[who]),
    ]

    def exchange(item, source, target):
        for df in range(1, feats):
            to = lax.rem(feat + df, feats)
            come = lax.rem(feat + feats - df, feats)
            copy = remote(
                source(to), target(feat), a_send.at[item, df], a_recv.at[item, df], node, to
            )
            copy.start()
            sent.append(copy)
            arrivals[item, df] = remote(
                source(to), target(come), a_send.at[item, df], a_recv.at[item, df], node, to
            )

    for item in (2, 3, 0):
        exchange(*groups[item])

    total = None
    for c in range(e1_chunks):
        e1_loads[c].wait()
        term = jnp.dot(
            feat_full[:, c * e1_rows : (c + 1) * e1_rows],
            edge1[c].astype(jnp.bfloat16),
            preferred_element_type=jnp.float32,
        )
        total = term if total is None else total + term
    agg_own[...] = (total / FAN1).astype(jnp.bfloat16)
    for copy in e2_loads:
        copy.start()
    for item in (1, 4, 5):
        exchange(*groups[item])

    def contract(weight, values):
        return lax.dot_general(
            weight, values, (((0,), (0,)), ((), ())), preferred_element_type=jnp.float32
        )

    before = contract(w1s_all[feat], feat_full[:, cols(feat)])
    before = before + contract(w1n_all[feat], agg_own[:, cols(feat)])
    for df in range(1, feats):
        come = lax.rem(feat + feats - df, feats)
        arrivals[0, df].wait_recv()
        arrivals[2, df].wait_recv()
        before = before + contract(w1s_all[come], feat_all[come])
        arrivals[1, df].wait_recv()
        arrivals[3, df].wait_recv()
        before = before + contract(w1n_all[come], agg_all[come])
    hidden = jnp.maximum(before, 0.0).astype(jnp.bfloat16)

    share = hidden.shape[0] // feats
    for df in range(1, feats):
        arrivals[4, df].wait_recv()
    projected = None
    for who in range(feats):
        term = jnp.dot(
            w2n_all[who],
            hidden[who * share : (who + 1) * share],
            preferred_element_type=jnp.float32,
        )
        projected = term if projected is None else projected + term
    p_all[node] = projected.astype(p_all.dtype)

    pl.when(odd == 1)(functools.partial(hear, 2 * (nodes - 1)))
    pl.when(odd == 0)(lambda: pl.semaphore_wait(ready, 1))
    p_arrive = {}
    for dn in range(1, nodes):
        to = lax.rem(node + dn, nodes)
        come = lax.rem(node + nodes - dn, nodes)
        copy = remote(p_all.at[node], p_all.at[node], p_send.at[dn], p_recv.at[dn], to, feat)
        copy.start()
        sent.append(copy)
        p_arrive[dn] = remote(
            p_all.at[node], p_all.at[come], p_send.at[dn], p_recv.at[dn], to, feat
        )

    for df in range(1, feats):
        arrivals[5, df].wait_recv()
    self_term = None
    for who in range(feats):
        term = jnp.dot(
            w2s_all[who],
            hidden[who * share : (who + 1) * share],
            preferred_element_type=jnp.float32,
        )
        self_term = term if self_term is None else self_term + term

    def gather(k, values):
        return jnp.dot(
            values, edge2[k].astype(jnp.bfloat16), preferred_element_type=jnp.float32
        )

    e2_loads[0].wait()
    gathered = gather(0, p_all[node])
    half = nodes // 2
    e2_loads[2].wait()
    p_arrive[1].wait_recv()
    gathered = gathered + gather(2, p_all[lax.rem(node + nodes - 1, nodes)])
    e2_loads[1].wait()
    if half != 1:
        p_arrive[half].wait_recv()
    gathered = gathered + gather(1, p_all[lax.rem(node + half, nodes)])
    for dn in range(1, nodes):
        if dn not in (1, half):
            p_arrive[dn].wait_recv()
    for k in range(3, slots):
        e2_loads[k].wait()
        values = p_all[need[0, k]]
        values = jnp.where(live[0, k] == 1, values, jnp.zeros_like(values))
        gathered = gathered + gather(k, values)
    part[...] = gathered

    c_arrive = {}
    for df in range(1, feats):
        to = lax.rem(feat + df, feats)
        come = lax.rem(feat + feats - df, feats)
        copy = remote(
            part.at[:, cols(to)], part_all.at[feat], c_send.at[df], c_recv.at[df], node, to
        )
        copy.start()
        sent.append(copy)
        c_arrive[df] = remote(
            part.at[:, cols(to)], part_all.at[come], c_send.at[df], c_recv.at[df], node, to
        )
    summed = part[:, cols(feat)]
    for df in range(1, feats):
        come = lax.rem(feat + feats - df, feats)
        c_arrive[df].wait_recv()
        summed = summed + part_all[come]
    logits = self_term + summed / FAN2
    class_ids = lax.broadcasted_iota(jnp.int32, logits.shape, 0)
    picked = jnp.sum(
        jnp.where(class_ids == lab[:, cols(feat)], logits, 0.0), axis=0, keepdims=True
    )
    loss = jnp.log(jnp.sum(jnp.exp(logits), axis=0, keepdims=True)) - picked
    mine = node * feats + feat
    loss_all[mine] = loss

    others = [(dn, df) for dn in range(nodes) for df in range(feats) if dn or df]
    d_arrive = []
    for index, (dn, df) in enumerate(others):
        to_node = lax.rem(node + dn, nodes)
        to_feat = lax.rem(feat + df, feats)
        come = lax.rem(node + nodes - dn, nodes) * feats + lax.rem(feat + feats - df, feats)
        copy = remote(
            loss_all.at[mine], loss_all.at[mine], d_send.at[index], d_recv.at[index], to_node, to_feat
        )
        copy.start()
        sent.append(copy)
        d_arrive.append(
            remote(
                loss_all.at[mine], loss_all.at[come], d_send.at[index], d_recv.at[index], to_node, to_feat
            )
        )
    for copy in d_arrive:
        copy.wait_recv()
    for who in range(feats):
        loss_out[:, who * quarter : (who + 1) * quarter] = loss_all[node * feats + who]
    total_loss = jnp.sum(loss_all[...])
    mean_out[0, 0] = total_loss / (block * nodes)
    for copy in sent:
        copy.wait_send()


def local(nodes, feats, features, edges_one, w1_self, w1_nbr, need, live, edges_two, w2_self, w2_nbr, labels):
    rows, block = features.shape
    hidden = w1_self.shape[1]
    share, classes = w2_self.shape
    quarter = block // feats
    slots = need.shape[1]
    chunks = 4
    ndev = nodes * feats
    bf16, f32, i32 = jnp.bfloat16, jnp.float32, jnp.int32
    anywhere = pl.BlockSpec(memory_space=pltpu.HBM)
    scalar = pl.BlockSpec(memory_space=pltpu.SMEM)
    sems = pltpu.SemaphoreType.DMA
    loss, mean = pl.pallas_call(
        functools.partial(kernel, nodes, feats),
        out_shape=(
            jax.ShapeDtypeStruct((1, block), f32),
            jax.ShapeDtypeStruct((1, 1), f32),
        ),
        in_specs=[
            anywhere,
            anywhere,
            anywhere,
            anywhere,
            scalar,
            scalar,
            anywhere,
            anywhere,
            anywhere,
            anywhere,
        ],
        out_specs=(pl.BlockSpec(memory_space=pltpu.VMEM), scalar),
        scratch_shapes=[
            pltpu.VMEM((rows, block), bf16),
            pltpu.VMEM((chunks, block // chunks, block), i32),
            pltpu.VMEM((slots, quarter, block), i32),
            pltpu.VMEM((1, block), i32),
            pltpu.VMEM((feats, rows, hidden), bf16),
            pltpu.VMEM((feats, rows, hidden), bf16),
            pltpu.VMEM((feats, classes, share), bf16),
            pltpu.VMEM((feats, classes, share), bf16),
            pltpu.VMEM((feats, rows, quarter), bf16),
            pltpu.VMEM((rows, block), bf16),
            pltpu.VMEM((feats, rows, quarter), bf16),
            pltpu.VMEM((nodes, classes, quarter), bf16),
            pltpu.VMEM((classes, block), f32),
            pltpu.VMEM((feats, classes, quarter), f32),
            pltpu.VMEM((ndev, 1, quarter), f32),
            sems((6,)),
            sems((chunks,)),
            sems((slots,)),
            sems((6, feats)),
            sems((6, feats)),
            sems((nodes,)),
            sems((nodes,)),
            sems((feats,)),
            sems((feats,)),
            sems((ndev,)),
            sems((ndev,)),
            pltpu.SemaphoreType.REGULAR,
        ],
        compiler_params=pltpu.CompilerParams(
            collective_id=0,
            has_side_effects=True,
        ),
    )(
        features,
        edges_one,
        w1_self,
        w1_nbr,
        need,
        live,
        edges_two,
        w2_self.T,
        w2_nbr.T,
        labels.reshape(1, block),
    )
    return loss.reshape(block), mean.reshape(())


def solution(mesh):
    return jax.shard_map(
        functools.partial(local, mesh.shape["node"], mesh.shape["feat"]),
        mesh=mesh,
        in_specs=(
            P("feat", "node"),
            P(None, "node"),
            P("feat", None),
            P("feat", None),
            P("node", None),
            P("node", None),
            P(None, "node"),
            P("feat", None),
            P("feat", None),
            P("node"),
        ),
        out_specs=(P("node"), P()),
        check_vma=False,
    )
```

```python
import functools

import jax
import jax.numpy as jnp
from jax import lax
from jax.experimental import pallas as pl
from jax.experimental.pallas import tpu as pltpu
from jax.sharding import PartitionSpec as P

FAN1 = 25
FAN2 = 10
MESH = pl.DeviceIdType.MESH


def kernel(
    nodes,
    feats,
    features,
    edges_one,
    w1_self,
    w1_nbr,
    need,
    live,
    edges_two,
    w2_self,
    w2_nbr,
    labels,
    loss_out,
    mean_out,
    feat_full,
    edge1,
    edge2,
    lab,
    w1s_all,
    w1n_all,
    w2s_all,
    w2n_all,
    feat_all,
    agg_own,
    agg_all,
    p_all,
    part,
    part_all,
    loss_all,
    load_sem,
    edge1_sem,
    edge2_sem,
    a_send,
    a_recv,
    p_send,
    p_recv,
    c_send,
    c_recv,
    d_send,
    d_recv,
    ready,
):
    node = lax.axis_index("node")
    feat = lax.axis_index("feat")
    block = feat_full.shape[1]
    quarter = block // feats
    slots = edges_two.shape[0] // block
    e1_chunks = edge1.shape[0]
    e1_rows = edge1.shape[1]

    def cols(index):
        return pl.ds(pl.multiple_of(index * quarter, quarter), quarter)

    def remote(src, dst, send, recv, node_id, feat_id):
        return pltpu.make_async_remote_copy(
            src_ref=src,
            dst_ref=dst,
            send_sem=send,
            recv_sem=recv,
            device_id={"node": node_id, "feat": feat_id},
            device_id_type=MESH,
        )

    loads = [
        pltpu.make_async_copy(features, feat_full, load_sem.at[0]),
        pltpu.make_async_copy(w1_self, w1s_all.at[feat], load_sem.at[1]),
        pltpu.make_async_copy(w1_nbr, w1n_all.at[feat], load_sem.at[2]),
        pltpu.make_async_copy(w2_self, w2s_all.at[feat], load_sem.at[3]),
        pltpu.make_async_copy(w2_nbr, w2n_all.at[feat], load_sem.at[4]),
        pltpu.make_async_copy(labels, lab, load_sem.at[5]),
    ]
    for copy in loads:
        copy.start()
    e1_loads = [
        pltpu.make_async_copy(
            edges_one.at[pl.ds(c * e1_rows, e1_rows), :], edge1.at[c], edge1_sem.at[c]
        )
        for c in range(e1_chunks)
    ]
    for copy in e1_loads:
        copy.start()
    e2_loads = [
        pltpu.make_async_copy(
            edges_two.at[pl.ds(pl.multiple_of(k * block + feat * quarter, quarter), quarter), :],
            edge2.at[k],
            edge2_sem.at[k],
        )
        for k in range(slots)
    ]
    barrier = pltpu.get_barrier_semaphore()
    odd = lax.rem(feat, 2)
    partner = feat + 1 - 2 * odd

    def greet(semaphore, to_node, to_feat):
        pl.semaphore_signal(
            semaphore,
            inc=1,
            device_id={"node": to_node, "feat": to_feat},
            device_id_type=MESH,
        )

    for df in range(1, feats):
        to = lax.rem(feat + df, feats)
        pl.when(lax.rem(to, 2) == 0)(functools.partial(greet, barrier, node, to))
    for dn in range(1, nodes):
        greet(barrier, lax.rem(node + dn, nodes), feat + 1 - odd)

    def hear(count):
        pl.semaphore_wait(barrier, count)
        greet(ready, node, partner)

    for copy in loads:
        copy.wait()
    pl.when(odd == 0)(functools.partial(hear, feats - 1))
    pl.when(odd == 1)(lambda: pl.semaphore_wait(ready, 1))

    sent = []
    arrivals = {}
    groups = [
        (0, lambda to: feat_full.at[:, cols(to)], lambda who: feat_all.at[who]),
        (1, lambda to: agg_own.at[:, cols(to)], lambda who: agg_all.at[who]),
        (2, lambda to: w1s_all.at[feat], lambda who: w1s_all.at[who]),
        (3, lambda to: w1n_all.at[feat], lambda who: w1n_all.at[who]),
        (4, lambda to: w2n_all.at[feat], lambda who: w2n_all.at[who]),
        (5, lambda to: w2s_all.at[feat], lambda who: w2s_all.at[who]),
    ]

    def exchange(item, source, target):
        for df in range(1, feats):
            to = lax.rem(feat + df, feats)
            come = lax.rem(feat + feats - df, feats)
            copy = remote(
                source(to), target(feat), a_send.at[item, df], a_recv.at[item, df], node, to
            )
            copy.start()
            sent.append(copy)
            arrivals[item, df] = remote(
                source(to), target(come), a_send.at[item, df], a_recv.at[item, df], node, to
            )

    for item in (2, 3, 0):
        exchange(*groups[item])

    total = None
    for c in range(e1_chunks):
        e1_loads[c].wait()
        term = jnp.dot(
            feat_full[:, c * e1_rows : (c + 1) * e1_rows],
            edge1[c].astype(jnp.bfloat16),
            preferred_element_type=jnp.float32,
        )
        total = term if total is None else total + term
    agg_own[...] = (total / FAN1).astype(jnp.bfloat16)
    for copy in e2_loads:
        copy.start()
    for item in (1, 4, 5):
        exchange(*groups[item])

    def contract(weight, values):
        return lax.dot_general(
            weight, values, (((0,), (0,)), ((), ())), preferred_element_type=jnp.float32
        )

    before = contract(w1s_all[feat], feat_full[:, cols(feat)])
    before = before + contract(w1n_all[feat], agg_own[:, cols(feat)])
    for df in range(1, feats):
        come = lax.rem(feat + feats - df, feats)
        arrivals[0, df].wait_recv()
        arrivals[2, df].wait_recv()
        before = before + contract(w1s_all[come], feat_all[come])
        arrivals[1, df].wait_recv()
        arrivals[3, df].wait_recv()
        before = before + contract(w1n_all[come], agg_all[come])
    hidden = jnp.maximum(before, 0.0).astype(jnp.bfloat16)

    share = hidden.shape[0] // feats
    for df in range(1, feats):
        arrivals[4, df].wait_recv()
    projected = None
    for who in range(feats):
        term = jnp.dot(
            w2n_all[who],
            hidden[who * share : (who + 1) * share],
            preferred_element_type=jnp.float32,
        )
        projected = term if projected is None else projected + term
    p_all[node] = projected.astype(p_all.dtype)

    pl.when(odd == 1)(functools.partial(hear, 2 * (nodes - 1)))
    pl.when(odd == 0)(lambda: pl.semaphore_wait(ready, 1))
    half = nodes // 2
    p_arrive = {}
    for dn in sorted(range(1, nodes), key=lambda d: abs(d - half)):
        to = lax.rem(node + dn, nodes)
        come = lax.rem(node + nodes - dn, nodes)
        copy = remote(p_all.at[node], p_all.at[node], p_send.at[dn], p_recv.at[dn], to, feat)
        copy.start()
        sent.append(copy)
        p_arrive[dn] = remote(
            p_all.at[node], p_all.at[come], p_send.at[dn], p_recv.at[dn], to, feat
        )

    for df in range(1, feats):
        arrivals[5, df].wait_recv()
    self_term = None
    for who in range(feats):
        term = jnp.dot(
            w2s_all[who],
            hidden[who * share : (who + 1) * share],
            preferred_element_type=jnp.float32,
        )
        self_term = term if self_term is None else self_term + term

    def gather(k, values):
        return jnp.dot(
            values, edge2[k].astype(jnp.bfloat16), preferred_element_type=jnp.float32
        )

    e2_loads[0].wait()
    gathered = gather(0, p_all[node])
    e2_loads[2].wait()
    p_arrive[1].wait_recv()
    gathered = gathered + gather(2, p_all[lax.rem(node + nodes - 1, nodes)])
    e2_loads[1].wait()
    if half != 1:
        p_arrive[half].wait_recv()
    gathered = gathered + gather(1, p_all[lax.rem(node + half, nodes)])
    for dn in range(1, nodes):
        if dn not in (1, half):
            p_arrive[dn].wait_recv()
    for k in range(3, slots):
        e2_loads[k].wait()
        values = p_all[need[0, k]]
        values = jnp.where(live[0, k] == 1, values, jnp.zeros_like(values))
        gathered = gathered + gather(k, values)
    part[...] = gathered

    c_arrive = {}
    for df in range(1, feats):
        to = lax.rem(feat + df, feats)
        come = lax.rem(feat + feats - df, feats)
        copy = remote(
            part.at[:, cols(to)], part_all.at[feat], c_send.at[df], c_recv.at[df], node, to
        )
        copy.start()
        sent.append(copy)
        c_arrive[df] = remote(
            part.at[:, cols(to)], part_all.at[come], c_send.at[df], c_recv.at[df], node, to
        )
    summed = part[:, cols(feat)]
    for df in range(1, feats):
        come = lax.rem(feat + feats - df, feats)
        c_arrive[df].wait_recv()
        summed = summed + part_all[come]
    logits = self_term + summed / FAN2
    class_ids = lax.broadcasted_iota(jnp.int32, logits.shape, 0)
    picked = jnp.sum(
        jnp.where(class_ids == lab[:, cols(feat)], logits, 0.0), axis=0, keepdims=True
    )
    loss = jnp.log(jnp.sum(jnp.exp(logits), axis=0, keepdims=True)) - picked
    mine = node * feats + feat
    loss_all[mine] = loss

    others = [(dn, df) for dn in range(nodes) for df in range(feats) if dn or df]
    d_arrive = []
    for index, (dn, df) in enumerate(others):
        to_node = lax.rem(node + dn, nodes)
        to_feat = lax.rem(feat + df, feats)
        come = lax.rem(node + nodes - dn, nodes) * feats + lax.rem(feat + feats - df, feats)
        copy = remote(
            loss_all.at[mine], loss_all.at[mine], d_send.at[index], d_recv.at[index], to_node, to_feat
        )
        copy.start()
        sent.append(copy)
        d_arrive.append(
            remote(
                loss_all.at[mine], loss_all.at[come], d_send.at[index], d_recv.at[index], to_node, to_feat
            )
        )
    for copy in d_arrive:
        copy.wait_recv()
    for who in range(feats):
        loss_out[:, who * quarter : (who + 1) * quarter] = loss_all[node * feats + who]
    total_loss = jnp.sum(loss_all[...])
    mean_out[0, 0] = total_loss / (block * nodes)
    for copy in sent:
        copy.wait_send()


def local(nodes, feats, features, edges_one, w1_self, w1_nbr, need, live, edges_two, w2_self, w2_nbr, labels):
    rows, block = features.shape
    hidden = w1_self.shape[1]
    share, classes = w2_self.shape
    quarter = block // feats
    slots = need.shape[1]
    chunks = 2
    ndev = nodes * feats
    bf16, f32, i32 = jnp.bfloat16, jnp.float32, jnp.int32
    anywhere = pl.BlockSpec(memory_space=pltpu.HBM)
    scalar = pl.BlockSpec(memory_space=pltpu.SMEM)
    sems = pltpu.SemaphoreType.DMA
    loss, mean = pl.pallas_call(
        functools.partial(kernel, nodes, feats),
        out_shape=(
            jax.ShapeDtypeStruct((1, block), f32),
            jax.ShapeDtypeStruct((1, 1), f32),
        ),
        in_specs=[
            anywhere,
            anywhere,
            anywhere,
            anywhere,
            scalar,
            scalar,
            anywhere,
            anywhere,
            anywhere,
            anywhere,
        ],
        out_specs=(pl.BlockSpec(memory_space=pltpu.VMEM), scalar),
        scratch_shapes=[
            pltpu.VMEM((rows, block), bf16),
            pltpu.VMEM((chunks, block // chunks, block), i32),
            pltpu.VMEM((slots, quarter, block), i32),
            pltpu.VMEM((1, block), i32),
            pltpu.VMEM((feats, rows, hidden), bf16),
            pltpu.VMEM((feats, rows, hidden), bf16),
            pltpu.VMEM((feats, classes, share), bf16),
            pltpu.VMEM((feats, classes, share), bf16),
            pltpu.VMEM((feats, rows, quarter), bf16),
            pltpu.VMEM((rows, block), bf16),
            pltpu.VMEM((feats, rows, quarter), bf16),
            pltpu.VMEM((nodes, classes, quarter), bf16),
            pltpu.VMEM((classes, block), f32),
            pltpu.VMEM((feats, classes, quarter), f32),
            pltpu.VMEM((ndev, 1, quarter), f32),
            sems((6,)),
            sems((chunks,)),
            sems((slots,)),
            sems((6, feats)),
            sems((6, feats)),
            sems((nodes,)),
            sems((nodes,)),
            sems((feats,)),
            sems((feats,)),
            sems((ndev,)),
            sems((ndev,)),
            pltpu.SemaphoreType.REGULAR,
        ],
        compiler_params=pltpu.CompilerParams(
            collective_id=0,
            has_side_effects=True,
        ),
    )(
        features,
        edges_one,
        w1_self,
        w1_nbr,
        need,
        live,
        edges_two,
        w2_self.T,
        w2_nbr.T,
        labels.reshape(1, block),
    )
    return loss.reshape(block), mean.reshape(())


def solution(mesh):
    return jax.shard_map(
        functools.partial(local, mesh.shape["node"], mesh.shape["feat"]),
        mesh=mesh,
        in_specs=(
            P("feat", "node"),
            P(None, "node"),
            P("feat", None),
            P("feat", None),
            P("node", None),
            P("node", None),
            P(None, "node"),
            P("feat", None),
            P("feat", None),
            P("node"),
        ),
        out_specs=(P("node"), P()),
        check_vma=False,
    )
```
